256 devices in a mesh: req: 64 (over x, y, z_hi), mesh: 4 (over z_lo, core).
Axes of the slice: x: 4, y: 4, z: 8 (z_hi: 4, z_lo: 2; z = z_hi * 2 + z_lo), core: 2. Of those that a mesh axis runs over, the one named last changes fastest.
Arguments:
- tokens: bfloat16 [1024, 64, 1024], P(('req', 'mesh')), may hold values from -6 to 6
- lengths: int32 [1024], P(('req', 'mesh')), may hold values from 1 to 64, 49152 in all
- ridge_keys: float32 [1024, 8, 128, 128], P(('req', 'mesh')), as said below
- ridge_values: float32 [1024, 8, 128, 128], P(('req', 'mesh')), may hold values from -0.5 to 0.5
- conv_tail: bfloat16 [1024, 3, 3072], P(('req', 'mesh')), may hold values from -6 to 6
- page_table: int32 [1024], P(('req', 'mesh')), may hold values from 0 to 15, as said below
- w_qkv: bfloat16 [1024, 3072], P(('req', 'mesh')), may hold values from -0.1875 to 0.1875
- conv_weight: float32 [4, 3072], replicated, may hold values from -3 to 3
- w_gates: bfloat16 [1024, 16], replicated, may hold values from -0.1875 to 0.1875
- decay_rate: float32 [8], replicated, may hold values from 0.001 to 0.03
- ridge: float32 [8], replicated, may hold values from 0.01 to 0.1
- w_out: bfloat16 [1024, 1024], P(('req', 'mesh')), may hold values from -0.1875 to 0.1875
- attn_gain: float32 [1024], replicated, may hold values from 0.5 to 1.5
- ffn_gain: float32 [1024], replicated, may hold values from 0.5 to 1.5
- w_gate: bfloat16 [1024, 2816], P('req', 'mesh'), may hold values from -0.1875 to 0.1875
- w_up: bfloat16 [1024, 2816], P('req', 'mesh'), may hold values from -0.1875 to 0.1875
- w_down: bfloat16 [2816, 1024], P('mesh', 'req'), may hold values from -0.109375 to 0.109375
Outputs:
- mixed: bfloat16 [1024, 64, 1024], P(('req', 'mesh'))
- keys_decode: float32 [1024, 8, 128, 128], P(('req', 'mesh'))
- values_decode: float32 [1024, 8, 128, 128], P(('req', 'mesh'))
- tail_decode: bfloat16 [1024, 3, 3072], P(('req', 'mesh'))
- readout: bfloat16 [1024, 64, 1024], P(('req', 'mesh'))
The draws below stay inside these ranges and needn't reach their ends.
Inputs may be any that keep to these rules, and one draw needn't show every extreme that they name: `page_table`: within each group of 16 consecutive requests the values are a permutation; value // 4 is a decode device of the group and value % 4 a slot on it, and the 4 requests of one device go to 4 different decode devices. `ridge_keys`: each matrix is symmetric with a positive diagonal that exceeds the sum of the magnitudes of its row's other entries.
All inputs are finite; a program needn't handle non-finite values. No bound on the sum of `lengths` on one device may be relied on, other than what follows from the above.
Results may differ from the reference program's by a relative error of at most 0.0095.
Values may be sent and summed in bfloat16 or wider, within the bound.
A program may use at most 128 MiB of HBM per device.

```python
import math
import jax
import jax.numpy as jnp
import numpy as np
from jax import lax

D = 1024
HEADS = 8
HEAD_DIM = 128
FF = 2816
CONV = 4
ITERS = 5
SPAN = 64
R_DEV = 4
REQS = 1024


def draw_ridge_keys(key, part):
    first_key, second_key = jax.random.split(jax.random.fold_in(key, 11))
    unit_off = jax.random.uniform(first_key, (REQS, HEADS, HEAD_DIM, HEAD_DIM), jnp.float32, -1.0, 1.0)
    unit_off = 0.5 * (unit_off + jnp.swapaxes(unit_off, 2, 3))
    fraction = jax.random.uniform(second_key, (REQS, HEADS, HEAD_DIM), jnp.float32)
    diagonal = 0.05 * jnp.exp(jnp.log(100.0) * fraction)
    smaller = jnp.minimum(diagonal[..., :, None], diagonal[..., None, :])
    symmetric = unit_off * smaller / HEAD_DIM
    position = jnp.arange(HEAD_DIM, dtype=jnp.int32)
    identity = position[:, None] == position[None, :]
    return jnp.where(identity, diagonal[..., :, None], symmetric)


def draw_page_table(key, part):
    group_count = REQS // (R_DEV * R_DEV)
    first_key, second_key = jax.random.split(jax.random.fold_in(key, 23))
    dest_keys = jax.random.split(first_key, group_count * R_DEV)
    slot_keys = jax.random.split(second_key, group_count * R_DEV)
    destination = jax.vmap(lambda one_key: jax.random.permutation(one_key, R_DEV))(dest_keys).reshape(group_count, R_DEV, R_DEV)
    slot_order = jax.vmap(lambda one_key: jax.random.permutation(one_key, R_DEV))(slot_keys).reshape(group_count, R_DEV, R_DEV)
    by_source = jnp.swapaxes(slot_order, 1, 2)
    slot_index = jnp.take_along_axis(by_source, destination, axis=2)
    return (destination * R_DEV + slot_index).reshape(REQS).astype(jnp.int32)


def steps_of(own_key, dims, shards, least, top_value):
    level, own = 1.0, jax.random.fold_in(own_key, 6)
    for axis_at, shards_of in shards:
        draws = jnp.exp(jax.random.uniform(jax.random.fold_in(own, axis_at), (shards_of,), jnp.float32, least / len(shards), top_value / len(shards)))
        level = level * jnp.repeat(draws, dims[axis_at] // shards_of).reshape([-1 if axis == axis_at else 1 for axis in range(len(dims))])
    return level


def split_up(number_of, total, most, lean):
    portions = [(1 << 20) // math.isqrt(grade ** lean) + 1 for grade in range(2, number_of + 1)]
    surplus, given = total - most - (number_of - 1), [1] * (number_of - 1)
    while surplus > 0:
        movable = [i for i in range(number_of - 1) if given[i] < most]
        whole, left = sum([portions[i] for i in movable]), surplus
        for i in movable:
            addition = min(most - given[i], max(1, left * portions[i] // whole), surplus)
            given[i] = given[i] + addition
            surplus = surplus - addition
    return np.array([most] + given)


def ragged_sizes(rng, number_of, total, reach, skew):
    if number_of == 2:
        one = jax.random.randint(rng, (), max(1, total - reach), min(reach, total - 1) + 1)
        return jnp.stack([one, total - one])
    sizes = jnp.asarray(split_up(number_of, total, reach, skew), jnp.int32)
    pairs = (number_of - 1) // 2
    source_of, taker = sizes[1:1 + 2 * pairs:2], sizes[2:2 + 2 * pairs:2]
    margin = jnp.minimum(source_of - 1, reach - taker)
    shifted = jax.random.randint(jax.random.fold_in(rng, 1), (pairs,), 0, 1 << 20) % (margin + 1)
    sizes = sizes.at[1:1 + 2 * pairs:2].set(source_of - shifted).at[2:2 + 2 * pairs:2].set(taker + shifted)
    return sizes[jax.random.permutation(jax.random.fold_in(rng, 2), number_of)]


def scatter_about(stream_key, extent, scale, most, pieces=(), held_as=jnp.bfloat16):
    array = scale * jax.random.normal(stream_key, extent, jnp.float32)
    if pieces:
        array = array * steps_of(stream_key, extent, pieces, -0.22, 0.18)
    return jnp.clip(array, -most, most).astype(held_as)


def setup_inputs(seed: int = 0) -> dict:
    streams_of = jax.random.split(jax.random.key(seed), 18)
    return {
        "tokens": scatter_about(streams_of[0], (REQS, SPAN, D), 1.0, 6.0, ((0, 256),)),
        "lengths": ragged_sizes(streams_of[1], REQS, REQS * SPAN * 3 // 4, SPAN, 2).astype(jnp.int32),
        "ridge_keys": draw_ridge_keys(jax.random.fold_in(streams_of[17], 71), 0),
        "ridge_values": scatter_about(streams_of[3], (REQS, HEADS, HEAD_DIM, HEAD_DIM), HEAD_DIM ** -0.5, 0.5, ((0, 256),), jnp.float32),
        "conv_tail": scatter_about(streams_of[4], (REQS, CONV - 1, 3 * HEADS * HEAD_DIM), 1.0, 6.0, ((0, 256),)),
        "page_table": draw_page_table(jax.random.fold_in(streams_of[17], 71), 0),
        "w_qkv": scatter_about(streams_of[6], (D, 3 * HEADS * HEAD_DIM), D ** -0.5, 0.1875, ((0, 256),)),
        "conv_weight": scatter_about(streams_of[7], (CONV, 3 * HEADS * HEAD_DIM), CONV ** -0.5, 3.0, (), jnp.float32),
        "w_gates": scatter_about(streams_of[8], (D, 2 * HEADS), D ** -0.5, 0.1875),
        "decay_rate": jnp.clip(jnp.exp(jax.random.uniform(streams_of[9], (HEADS,), jnp.float32, math.log(0.001), math.log(0.03))), 0.001, 0.03),
        "ridge": jnp.clip(jnp.exp(jax.random.uniform(streams_of[10], (HEADS,), jnp.float32, math.log(0.01), math.log(0.1))), 0.01, 0.1),
        "w_out": scatter_about(streams_of[11], (HEADS * HEAD_DIM, D), (HEADS * HEAD_DIM) ** -0.5, 0.1875, ((0, 256),)),
        "attn_gain": jnp.clip(1.0 + 0.1 * jax.random.normal(streams_of[12], (D,), jnp.float32), 0.5, 1.5),
        "ffn_gain": jnp.clip(1.0 + 0.1 * jax.random.normal(streams_of[13], (D,), jnp.float32), 0.5, 1.5),
        "w_gate": scatter_about(streams_of[14], (D, FF), D ** -0.5, 0.1875, ((0, 64), (1, 4))),
        "w_up": scatter_about(streams_of[15], (D, FF), D ** -0.5, 0.1875, ((0, 64), (1, 4))),
        "w_down": scatter_about(streams_of[16], (FF, D), FF ** -0.5, 0.109375, ((0, 4), (1, 64))),
    }


def rms_norm(values, gain):
    return values * lax.rsqrt(lax.optimization_barrier(jnp.mean(values * values, axis=-1, keepdims=True)) + 1e-05) * gain

def unit_rows(values):
    return values * lax.rsqrt(lax.optimization_barrier(jnp.sum(values * values, axis=-1, keepdims=True)) + 1e-06)

def prepare_heads(projected, gate_logits, conv_tail, lengths, conv_weight, decay_rate):
    requests, length, columns = projected.shape
    heads = decay_rate.shape[0]
    window = conv_tail.shape[1]
    extended = jnp.concatenate([conv_tail, projected], axis=1)
    conv_sum = jnp.zeros((requests, length, columns), jnp.float32)
    for tap_index in range(window + 1):
        conv_sum = conv_sum + conv_weight[tap_index] * extended[:, tap_index:tap_index + length].astype(jnp.float32)
    activated = jax.nn.silu(conv_sum).reshape(requests, length, 3, heads, columns // (3 * heads))
    queries = unit_rows(activated[:, :, 0])
    keys_now = unit_rows(activated[:, :, 1])
    values_now = activated[:, :, 2]
    position = jnp.arange(length, dtype=jnp.int32)
    live = (position[None, :] < lengths[:, None]).astype(jnp.float32)[:, :, None]
    beta = jax.nn.sigmoid(gate_logits[..., 0]) * live
    log_decay = -decay_rate * jax.nn.softplus(gate_logits[..., 1]) * live
    new_tail = jax.vmap(lambda rows_all, first_row: lax.dynamic_slice_in_dim(rows_all, first_row, window, 0))(extended, lengths.astype(jnp.int32))
    return (queries, keys_now, values_now, beta, log_decay, new_tail)

def mesa_core(queries, keys_now, values_now, beta, log_decay, keys_start, values_start, ridge, iterations):
    highest = lax.Precision.HIGHEST
    cumulative = jnp.cumsum(jnp.swapaxes(log_decay, 1, 2), axis=-1)
    beta_heads = jnp.swapaxes(beta, 1, 2)
    length = cumulative.shape[-1]
    position = jnp.arange(length, dtype=jnp.int32)
    causal = position[:, None] >= position[None, :]
    spread = cumulative[..., :, None] - cumulative[..., None, :]
    weight = jnp.where(causal, jnp.exp(jnp.minimum(spread, 0.0)), 0.0) * beta_heads[..., None, :]
    carried = jnp.swapaxes(jnp.exp(cumulative), 1, 2)[..., None]
    ridge_term = ridge[None, None, :, None]

    def apply_system(field):
        start_part = carried * jnp.einsum('bthj,bhij->bthi', field, keys_start, precision=highest)
        scores = jnp.einsum('bthj,bshj->bhts', field, keys_now, precision=highest) * weight
        return start_part + jnp.einsum('bhts,bshj->bthj', scores, keys_now, precision=highest) + ridge_term * field
    solution = jnp.zeros_like(queries)
    residual = queries
    direction = queries
    res_norm = lax.optimization_barrier(jnp.sum(residual * residual, axis=-1, keepdims=True))
    for step_index in range(iterations):
        applied = apply_system(direction)
        step_size = res_norm / (lax.optimization_barrier(jnp.sum(direction * applied, axis=-1, keepdims=True)) + 1e-20)
        solution = solution + step_size * direction
        residual = residual - step_size * applied
        next_norm = lax.optimization_barrier(jnp.sum(residual * residual, axis=-1, keepdims=True))
        direction = residual + next_norm / (res_norm + 1e-20) * direction
        res_norm = next_norm
    read_start = carried * jnp.einsum('bthj,bhij->bthi', solution, values_start, precision=highest)
    scores = jnp.einsum('bthj,bshj->bhts', solution, keys_now, precision=highest) * weight
    readout = read_start + jnp.einsum('bhts,bshj->bthj', scores, values_now, precision=highest)
    tail_weight = jnp.swapaxes(jnp.exp(cumulative[..., -1:] - cumulative) * beta_heads, 1, 2)[..., None]
    final_decay = jnp.exp(cumulative[..., -1])[..., None, None]
    keys_end = final_decay * keys_start + jnp.einsum('bshi,bshj->bhij', keys_now * tail_weight, keys_now, precision=highest)
    values_end = final_decay * values_start + jnp.einsum('bshi,bshj->bhij', values_now * tail_weight, keys_now, precision=highest)
    return (readout, keys_end, values_end)

def layer_forward(tokens, lengths, keys_start, values_start, conv_tail, w_qkv, conv_weight, w_gates, decay_rate, ridge, w_out, attn_gain, ffn_gain, w_gate, w_up, w_down):
    requests, length, width = tokens.shape
    heads = decay_rate.shape[0]
    resident = tokens.astype(jnp.float32).reshape(requests * length, width)
    normed = rms_norm(resident, attn_gain).astype(jnp.bfloat16)
    projected = jnp.dot(normed, w_qkv, preferred_element_type=jnp.float32).astype(jnp.bfloat16).reshape(requests, length, -1)
    gate_logits = jnp.dot(normed, w_gates, preferred_element_type=jnp.float32).reshape(requests, length, heads, 2)
    queries, keys_now, values_now, beta, log_decay, new_tail = prepare_heads(projected, gate_logits, conv_tail, lengths, conv_weight, decay_rate)
    readout, keys_end, values_end = mesa_core(queries, keys_now, values_now, beta, log_decay, keys_start, values_start, ridge, ITERS)
    head_rows = readout.reshape(requests * length, -1).astype(jnp.bfloat16)
    attended = jnp.dot(head_rows, w_out, preferred_element_type=jnp.float32)
    after_attn = (resident + attended).astype(jnp.bfloat16)
    ffn_in = rms_norm(after_attn.astype(jnp.float32), ffn_gain).astype(jnp.bfloat16)
    gate_proj = jnp.dot(ffn_in, w_gate, preferred_element_type=jnp.float32)
    upward = jnp.dot(ffn_in, w_up, preferred_element_type=jnp.float32)
    hidden = (jax.nn.silu(gate_proj) * upward).astype(jnp.bfloat16)
    ffn_out = jnp.dot(hidden, w_down, preferred_element_type=jnp.float32)
    mixed = (after_attn.astype(jnp.float32) + ffn_out).astype(jnp.bfloat16).reshape(requests, length, width)
    return (mixed, keys_end, values_end, new_tail, head_rows.reshape(requests, length, -1))

def reference(tokens, lengths, ridge_keys, ridge_values, conv_tail, page_table, w_qkv, conv_weight, w_gates, decay_rate, ridge, w_out, attn_gain, ffn_gain, w_gate, w_up, w_down):
    block_size = 8
    block_count = REQS // block_size

    def split_blocks(values):
        return values.reshape((block_count, block_size) + values.shape[1:])

    def merge_blocks(values):
        return values.reshape((REQS,) + values.shape[2:])

    def one_block(block_items):
        tok_block, len_block, keys_block, vals_block, tail_block = block_items
        return layer_forward(tok_block, len_block, keys_block, vals_block, tail_block, w_qkv, conv_weight, w_gates, decay_rate, ridge, w_out, attn_gain, ffn_gain, w_gate, w_up, w_down)
    mixed, keys_end, values_end, new_tail, readout = lax.map(one_block, (split_blocks(tokens), split_blocks(lengths), split_blocks(ridge_keys), split_blocks(ridge_values), split_blocks(conv_tail)))
    mixed = merge_blocks(mixed)
    keys_end = merge_blocks(keys_end)
    values_end = merge_blocks(values_end)
    new_tail = merge_blocks(new_tail)
    readout = merge_blocks(readout)
    group_size = R_DEV * R_DEV
    target = jnp.arange(REQS, dtype=jnp.int32) // group_size * group_size + page_table.astype(jnp.int32)
    keys_decode = jnp.zeros_like(keys_end).at[target].set(keys_end)
    values_decode = jnp.zeros_like(values_end).at[target].set(values_end)
    tail_decode = jnp.zeros_like(new_tail).at[target].set(new_tail)
    return (mixed, keys_decode, values_decode, tail_decode, readout)
```

```python
import functools

import jax
import jax.numpy as jnp
from jax import lax
from jax.experimental import pallas as pl
from jax.experimental.pallas import tpu as pltpu
from jax.sharding import PartitionSpec as P

ITERS = 5
MESH = pl.DeviceIdType.MESH
ANY = pl.BlockSpec(memory_space=pl.ANY)
VMEM = pl.BlockSpec(memory_space=pltpu.VMEM)
NX, NY, NZ, ZH = 4, 4, 8, 4
ALL = None


def place_of():
    req = lax.axis_index("req")
    peer = lax.axis_index("mesh")
    x = req // (NY * ZH)
    y = (req // ZH) % NY
    z = (req % ZH) * 2 + peer // 2
    return x, y, z, peer % 2


def device_of(x, y, z, core):
    return ((x * NY + y) * ZH + z // 2, (z % 2) * 2 + core)


def slab(ref, core, x, y, z, half=None):
    lo, hi = (slice(0, 2), slice(0, ZH)) if z is ALL else (z % 2, z // 2)
    xs = slice(0, NX) if x is ALL else x
    ys = slice(0, NY) if y is ALL else y
    if half is not None:
        if z is ALL:
            lo = slice(half, half + 1)
        else:
            xs = slice(2 * half, 2 * half + 2)
    return ref.at[core, lo, xs, ys, hi]


class Gather:
    def __init__(self, dest, order, sems, base, me):
        self.dest, self.order, self.sems, self.next, self.me = dest, order, sems, base, me
        self.sent = []

    def send(self, where, target):
        x, y, z, core = target
        at = self.next
        self.next += 1
        copy = pltpu.make_async_remote_copy(
            src_ref=where,
            dst_ref=where,
            send_sem=self.sems.at[0, at],
            recv_sem=self.sems.at[1, at],
            device_id=device_of(x, y, z, core),
            device_id_type=MESH,
        )
        copy.start()
        self.sent.append(copy)
        return at

    def arrive(self, where, at):
        pltpu.make_async_remote_copy(
            src_ref=where,
            dst_ref=where,
            send_sem=self.sems.at[0, at],
            recv_sem=self.sems.at[1, at],
            device_id=device_of(*self.me),
            device_id_type=MESH,
        ).wait_recv()

    def moved(self, axis, by):
        place = list(self.me)
        size = (NX, NY, NZ)[axis]
        place[axis] = lax.rem(place[axis] + by + size, size)
        return tuple(place)

    def part(self, axis, by, done, half=None, core=None):
        place = list(self.moved(axis, by))
        for each in done:
            place[each] = ALL
        x, y, z, own = place
        return slab(self.dest, own if core is None else core, x, y, z, half)

    def partner(self):
        x, y, z, core = self.me
        return (x, y, z, 1 - core)

    def stages(self):
        out = []
        first, second, third = self.order
        state = {}

        def direct():
            size = (NX, NY, NZ)[first]
            state["first"] = [
                (by, self.send(self.part(first, 0, ()), self.moved(first, by)))
                for by in range(1, size)
            ]

        def ring(axis, done, last):
            size = (NX, NY, NZ)[axis]
            far = size // 2
            tag = ("ring", axis)

            def cross(by, half):
                if last:
                    at = self.send(self.part(axis, by, done, half), self.partner())
                    state.setdefault("cross", []).append((by, half, at))

            def begin():
                here = self.part(axis, 0, done)
                state[tag] = [
                    (self.send(here, self.moved(axis, 1)), self.send(here, self.moved(axis, -1)))
                ]
                cross(0, None)

            def middle(step):
                right, left = state[tag][-1]
                cut = step == far - 1
                self.arrive(self.part(axis, -step, done), right)
                at_right = self.send(
                    self.part(axis, -step, done, 0 if cut else None), self.moved(axis, 1)
                )
                self.arrive(self.part(axis, step, done), left)
                at_left = self.send(
                    self.part(axis, step, done, 1 if cut else None), self.moved(axis, -1)
                )
                state[tag].append((at_right, at_left))
                cross(-step, None)
                cross(step, None)

            def end():
                right, left = state[tag][-1]
                self.arrive(self.part(axis, far, done, 0), right)
                cross(far, 0)
                self.arrive(self.part(axis, far, done, 1), left)
                cross(far, 1)

            return begin, [functools.partial(middle, s) for s in range(1, far)], end

        b2, m2, e2 = ring(second, (first,), False)
        b3, m3, e3 = ring(third, (first, second), True)

        def after_first():
            for by, at in state["first"]:
                self.arrive(self.part(first, -by, ()), at)
            b2()

        def after_second():
            e2()
            b3()

        def after_cross():
            for by, half, at in state["cross"]:
                self.arrive(
                    self.part(third, by, (first, second), half, core=1 - self.me[3]), at
                )
            for copy in self.sent:
                copy.wait_send()

        out.append(direct)
        out.append(after_first)
        out.extend(m2)
        out.append(after_second)
        out.extend(m3)
        out.append(e3)
        out.append(after_cross)
        return out


COPIES = 26
XYZ, ZYX, ZXY = (0, 1, 2), (2, 1, 0), (2, 0, 1)


def enter(me, group=True):
    barrier = pltpu.get_barrier_semaphore()
    x, y, z, core = me
    others = [(lax.rem(x + by, NX), y, z, core) for by in range(1, NX)]
    others += [(x, lax.rem(y + by, NY), z, core) for by in range(1, NY)]
    others += [(x, y, lax.rem(z + by, NZ), core) for by in range(1, NZ)]
    others += [(x, y, z, 1 - core)]
    if group:
        pair = (z // 2) * 2 + 1 - z % 2
        others += [(x, y, pair, 1 - core)]
    for other in others:
        pl.semaphore_signal(barrier, inc=1, device_id=device_of(*other), device_id_type=MESH)
    pl.semaphore_wait(barrier, len(others))


def run_stages(jobs):
    lists = [job.stages() for job in jobs]
    for step in range(max(len(each) for each in lists)):
        for each in lists:
            if step < len(each):
                each[step]()


def gather_kernel(
    pieces_ref, pages_ref, gate_ref, up_ref, down_ref,
    qa, qb, qc, wo, wg, wu, wd, pages_out,
    landed, rows, stage, sems, group_sems, local_sems,
):
    me = place_of()
    x, y, z, core = me
    req, peer = lax.axis_index("req"), lax.axis_index("mesh")
    enter(me)
    early = []
    for by in range(1, 4):
        other = lax.rem(peer + by, 4)
        for what, (src, dst) in enumerate(
            (
                (pieces_ref.at[other], landed.at[peer]),
                (pages_ref, pages_out.at[peer]),
            )
        ):
            copy = pltpu.make_async_remote_copy(
                src_ref=src,
                dst_ref=dst,
                send_sem=group_sems.at[0, what, by],
                recv_sem=group_sems.at[1, what, by],
                device_id=(req, other),
                device_id_type=MESH,
            )
            copy.start()
            early.append(copy)
    lo, hi = z % 2, z // 2
    own = [
        pltpu.make_async_copy(pages_ref, pages_out.at[peer], local_sems.at[0]),
        pltpu.make_async_copy(gate_ref, wg.at[core, lo, x, y, hi], local_sems.at[1]),
        pltpu.make_async_copy(up_ref, wu.at[core, lo, x, y, hi], local_sems.at[2]),
        pltpu.make_async_copy(down_ref, wd.at[core, lo, x, y, hi], local_sems.at[3]),
        pltpu.make_async_copy(pieces_ref.at[peer], landed.at[peer], local_sems.at[4]),
    ]
    for copy in own:
        copy.start()
    own[4].wait()
    for by in range(1, 4):
        source = lax.rem(peer + 4 - by, 4)
        for what, where in enumerate((landed.at[source], pages_out.at[source])):
            pltpu.make_async_remote_copy(
                src_ref=where,
                dst_ref=where,
                send_sem=group_sems.at[0, what, by],
                recv_sem=group_sems.at[1, what, by],
                device_id=(req, peer),
                device_id_type=MESH,
            ).wait_recv()
    for source in range(4):
        rows[4 * source : 4 * source + 4, :] = landed[source].astype(jnp.float32)
    stage[...] = rows[...].astype(jnp.bfloat16)
    blocks = [
        pltpu.make_async_copy(
            stage.at[:, 256 * n : 256 * n + 256],
            ref.at[core, lo, x, y, hi],
            local_sems.at[5 + n],
        )
        for n, ref in enumerate((qa, qb, qc, wo))
    ]
    for copy in blocks:
        copy.start()
    for copy in blocks:
        copy.wait()
    for copy in own[:4]:
        copy.wait()
    run_stages(
        [
            Gather(ref, order, sems.at[n], 0, me)
            for n, (ref, order) in enumerate(
                (
                    (qa, XYZ), (qb, ZYX), (qc, ZXY), (wg, XYZ), (wu, ZYX), (wd, ZXY), (wo, ZXY),
                )
            )
        ]
    )
    for copy in early:
        copy.wait_send()


def gather_all(pieces, pages, gate, up, down):
    grid = (2, 2, NX, NY, ZH, 16)

    def block(n):
        return jax.ShapeDtypeStruct(grid + (n,), jnp.bfloat16)

    ff = gate.shape[1]
    return pl.pallas_call(
        gather_kernel,
        name="gather_weights",
        out_shape=[block(256)] * 4
        + [block(ff)] * 3
        + [jax.ShapeDtypeStruct((4,) + pages.shape, jnp.int32)],
        in_specs=[VMEM] * 5,
        out_specs=[ANY] * 8,
        scratch_shapes=[
            pltpu.VMEM((4, 4, 1024), jnp.bfloat16),
            pltpu.VMEM((16, 1024), jnp.float32),
            pltpu.VMEM((16, 1024), jnp.bfloat16),
            pltpu.SemaphoreType.DMA((7, 2, COPIES)),
            pltpu.SemaphoreType.DMA((2, 2, 4)),
            pltpu.SemaphoreType.DMA((9,)),
        ],
        compiler_params=pltpu.CompilerParams(collective_id=0, has_side_effects=True),
    )(pieces, pages, gate, up, down)


def split2(value):
    high = value.astype(jnp.bfloat16)
    low = (value - high.astype(jnp.float32)).astype(jnp.bfloat16)
    return jnp.concatenate([high, low], axis=0)


def dot(a, b, contract=((1,), (0,)), precision=None):
    return lax.dot_general(
        a, b, (contract, ((), ())), preferred_element_type=jnp.float32, precision=precision
    )


def dot2(stacked, b, contract=((1,), (0,))):
    both = dot(stacked, b, contract)
    half = both.shape[0] // 2
    return both[:half] + both[half:]


def rms_norm(values, gain):
    return values * lax.rsqrt(jnp.mean(values * values, axis=-1, keepdims=True) + 1e-05) * gain


def mesa_kernel(
    lengths, dest, ridge,
    tokens, w_gates, gain, rate, rate_col, conv_weight, tail, keys0, values0, qa, qb, qc,
    readout, send_keys, send_values, send_tail,
    normed, projected, extended, act,
):
    r = pl.program_id(0)
    high = lax.Precision.HIGHEST

    @pl.when(r == 0)
    def _():
        normed[...] = rms_norm(tokens[...].astype(jnp.float32), gain[...]).astype(jnp.bfloat16)
        for core in range(2):
            for lo in range(2):
                for n, ref in enumerate((qa, qb, qc)):
                    at = (lo * 2 + core) * 768 + n * 256
                    projected[:, at : at + 256] = dot(
                        normed[...], ref[core * 2 + lo]
                    ).astype(jnp.bfloat16)

    length = lengths[r]
    mine = pl.ds(pl.multiple_of(r * 64, 64), 64)
    extended[5:8, :] = tail[0].astype(jnp.float32)
    extended[8:72, :] = projected[mine, :].astype(jnp.float32)
    from_row = 5 + length
    window = extended[pl.ds(pl.multiple_of(from_row // 8 * 8, 8), 16), :]
    send_tail[0] = pltpu.roll(window, (16 - from_row % 8) % 16, 0)[:3].astype(jnp.bfloat16)
    total = conv_weight[0:1, :] * extended[5:69, :]
    for tap in range(1, 4):
        total = total + conv_weight[tap : tap + 1, :] * extended[5 + tap : 69 + tap, :]
    act[...] = total * jax.nn.sigmoid(total)

    logits = dot(normed[mine, :], w_gates[...])
    pick_row = lax.broadcasted_iota(jnp.int32, (16, 8), 0)
    pick_col = lax.broadcasted_iota(jnp.int32, (16, 8), 1)
    in_logit = dot(logits, (pick_row == 2 * pick_col).astype(jnp.float32), precision=high)
    out_logit = dot(logits, (pick_row == 2 * pick_col + 1).astype(jnp.float32), precision=high)
    slot = lax.broadcasted_iota(jnp.int32, (64, 8), 0)
    live = (slot < length).astype(jnp.float32)
    beta = jax.nn.sigmoid(in_logit) * live
    log_decay = -rate[...] * jax.nn.softplus(out_logit) * live
    t_at = lax.broadcasted_iota(jnp.int32, (64, 64), 0)
    s_at = lax.broadcasted_iota(jnp.int32, (64, 64), 1)
    causal = s_at <= t_at
    lower = causal.astype(jnp.float32)
    same = (t_at == s_at).astype(jnp.float32)
    cum = dot(lower, log_decay, precision=high)
    cum_rows = dot(cum, same, ((0,), (0,)), precision=high)
    beta_rows = dot(beta, same, ((0,), (0,)), precision=high)
    carried_all = jnp.exp(cum)

    for first in range(0, 8, HEADS_AT_ONCE):
        heads = range(first, first + HEADS_AT_ONCE)
        states = []
        for h in heads:
            q = act[:, h * 128 : h * 128 + 128]
            k = act[:, 1024 + h * 128 : 1152 + h * 128]
            v = act[:, 2048 + h * 128 : 2176 + h * 128]
            q = q * lax.rsqrt(jnp.sum(q * q, axis=-1, keepdims=True) + 1e-06)
            k = k * lax.rsqrt(jnp.sum(k * k, axis=-1, keepdims=True) + 1e-06)
            cum_col, cum_row = cum[:, h : h + 1], cum_rows[h : h + 1, :]
            beta_row = beta_rows[h : h + 1, :]
            spread = jnp.exp(jnp.minimum(cum_col - cum_row, 0.0))
            weight = jnp.where(causal, spread, 0.0) * beta_row
            last = cum[63:64, h : h + 1]
            final = jnp.exp(last)
            tail_row = jnp.exp(last - cum_row) * beta_row
            k_b = k.astype(jnp.bfloat16)
            k_t, v_t = k.T, v.T
            start_k, start_v = keys0[0, h], values0[0, h]
            send_keys[0, h] = (
                final * start_k + dot2(split2(k_t * tail_row), k_b)
            ).astype(jnp.bfloat16)
            send_values[0, h] = (
                final * start_v + dot2(split2(v_t * tail_row), k_b)
            ).astype(jnp.bfloat16)
            right = jnp.concatenate(
                [start_k.astype(jnp.bfloat16), k_t.astype(jnp.bfloat16)], axis=1
            )
            states.append(
                dict(
                    x=jnp.zeros_like(q), res=q, p=q, rr=jnp.sum(q * q, axis=-1, keepdims=True),
                    right=right, k_b=k_b, k_tb=k_t.astype(jnp.bfloat16), v_b=v.astype(jnp.bfloat16),
                    v0=start_v.astype(jnp.bfloat16), weight=weight,
                    carried=carried_all[:, h : h + 1], ridge=ridge[h],
                )
            )
        for _ in range(ITERS):
            for s in states:
                both = dot2(split2(s["p"]), s["right"])
                s["start"] = s["carried"] * both[:, :128]
                s["scores"] = both[:, 128:] * s["weight"]
            for s in states:
                applied = (
                    s["start"] + dot2(split2(s["scores"]), s["k_b"]) + s["ridge"] * s["p"]
                )
                step = s["rr"] / (jnp.sum(s["p"] * applied, axis=-1, keepdims=True) + 1e-20)
                s["x"] = s["x"] + step * s["p"]
                s["res"] = s["res"] - step * applied
                after = jnp.sum(s["res"] * s["res"], axis=-1, keepdims=True)
                s["p"] = s["res"] + after / (s["rr"] + 1e-20) * s["p"]
                s["rr"] = after
        for h, s in zip(heads, states):
            stacked = split2(s["x"])
            start = s["carried"] * dot2(stacked, s["v0"], ((1,), (1,)))
            scores = dot2(stacked, s["k_tb"]) * s["weight"]
            readout[:, h * 128 : h * 128 + 128] = (
                start + dot2(split2(scores), s["v_b"])
            ).astype(jnp.bfloat16)


HEADS_AT_ONCE = 4


def mesa(lengths, dest, ridge, tokens, w_gates, gain, rate, conv_weight, tail, keys0, values0, qs):
    def whole(shape):
        return pl.BlockSpec(shape, lambda r, *_: (0,) * len(shape))

    def by_request(shape):
        return pl.BlockSpec(shape, lambda r, *_: (r,) + (0,) * (len(shape) - 1))

    def by_dest(shape):
        return pl.BlockSpec(shape, lambda r, n, d, *_: (d[r],) + (0,) * (len(shape) - 1))

    state = (1, 8, 128, 128)
    return pl.pallas_call(
        mesa_kernel,
        name="mesa",
        grid_spec=pltpu.PrefetchScalarGridSpec(
            num_scalar_prefetch=3,
            grid=(4,),
            in_specs=[
                whole((256, 1024)), whole((1024, 16)), whole((1, 1024)), whole((1, 8)),
                whole((8, 1)), whole((4, 3072)), by_request((1, 3, 3072)), by_request(state),
                by_request(state), whole((4, 1024, 256)), whole((4, 1024, 256)),
                whole((4, 1024, 256)),
            ],
            out_specs=[
                by_request((64, 1024)), by_dest(state), by_dest(state), by_dest((1, 3, 3072)),
            ],
            scratch_shapes=[
                pltpu.VMEM((256, 1024), jnp.bfloat16),
                pltpu.VMEM((256, 3072), jnp.bfloat16),
                pltpu.VMEM((80, 3072), jnp.float32),
                pltpu.VMEM((64, 3072), jnp.float32),
            ],
        ),
        out_shape=[
            jax.ShapeDtypeStruct((256, 1024), jnp.bfloat16),
            jax.ShapeDtypeStruct((4, 8, 128, 128), jnp.bfloat16),
            jax.ShapeDtypeStruct((4, 8, 128, 128), jnp.bfloat16),
            jax.ShapeDtypeStruct((4, 3, 3072), jnp.bfloat16),
        ],
        compiler_params=pltpu.CompilerParams(vmem_limit_bytes=60 << 20),
    )(
        lengths, dest, ridge, tokens, w_gates, gain, rate, rate.reshape(8, 1), conv_weight, tail,
        keys0, values0, *qs,
    )


def handover_kernel(keys, values, tails, got_keys, got_values, got_tails, sems):
    req, peer = lax.axis_index("req"), lax.axis_index("mesh")
    barrier = pltpu.get_barrier_semaphore()
    for by in range(1, 4):
        pl.semaphore_signal(
            barrier, inc=1, device_id=(req, lax.rem(peer + by, 4)), device_id_type=MESH
        )
    pl.semaphore_wait(barrier, 3)
    copies = []
    for by in range(1, 4):
        other = lax.rem(peer + by, 4)
        for n, (src, dst) in enumerate(
            ((keys, got_keys), (values, got_values), (tails, got_tails))
        ):
            copy = pltpu.make_async_remote_copy(
                src_ref=src.at[other],
                dst_ref=dst.at[peer],
                send_sem=sems.at[0, by, n],
                recv_sem=sems.at[1, by, n],
                device_id=(req, other),
                device_id_type=MESH,
            )
            copy.start()
            copies.append(copy)
    for by in range(1, 4):
        source = lax.rem(peer + 4 - by, 4)
        for n, dst in enumerate((got_keys, got_values, got_tails)):
            pltpu.make_async_remote_copy(
                src_ref=dst.at[source],
                dst_ref=dst.at[source],
                send_sem=sems.at[0, by, n],
                recv_sem=sems.at[1, by, n],
                device_id=(req, peer),
                device_id_type=MESH,
            ).wait_recv()
    for copy in copies:
        copy.wait_send()


def handover(keys, values, tails):
    return pl.pallas_call(
        handover_kernel,
        name="handover",
        out_shape=[jax.ShapeDtypeStruct(a.shape, a.dtype) for a in (keys, values, tails)],
        in_specs=[ANY] * 3,
        out_specs=[ANY] * 3,
        scratch_shapes=[pltpu.SemaphoreType.DMA((2, 4, 3))],
        compiler_params=pltpu.CompilerParams(collective_id=1, has_side_effects=True),
    )(keys, values, tails)


def finish_kernel(
    slots, me,
    readout, tokens, gain, w_out, w_gate, w_up, w_down,
    got_keys, got_values, got_tails, own_keys, own_values, own_tails,
    mixed, keys, values, tails,
    after, ffn_in, total,
):
    q = pl.program_id(0)

    @pl.when(q == 0)
    def _():
        for core in range(2):
            for lo in range(2):
                at = (lo * 2 + core) * 256
                after[:, at : at + 256] = (
                    tokens[:, at : at + 256].astype(jnp.float32)
                    + dot(readout[...], w_out[core * 2 + lo])
                ).astype(jnp.bfloat16).astype(jnp.float32)
        ffn_in[...] = rms_norm(after[...], gain[...]).astype(jnp.bfloat16)

    gate = dot(ffn_in[...], w_gate[0])
    hidden = (gate * jax.nn.sigmoid(gate) * dot(ffn_in[...], w_up[0])).astype(jnp.bfloat16)
    part = dot(hidden, w_down[0], ((1,), (1,)))

    @pl.when(q == 0)
    def _():
        total[...] = part

    @pl.when(jnp.logical_and(q > 0, q < 3))
    def _():
        total[...] += part

    @pl.when(q == 3)
    def _():
        mixed[...] = (after[...] + (total[...] + part)).astype(jnp.bfloat16)

    mine = me[0] == q
    keys[...] = jnp.where(mine, own_keys[...], got_keys[...]).astype(jnp.float32)
    values[...] = jnp.where(mine, own_values[...], got_values[...]).astype(jnp.float32)
    tails[...] = jnp.where(mine, own_tails[...], got_tails[...])


def finish(slots, me, readout, tokens, gain, w_out, w_gate, w_up, w_down, got, own):
    def whole(shape):
        return pl.BlockSpec(shape, lambda q, *_: (0,) * len(shape))

    def by_step(shape):
        return pl.BlockSpec(shape, lambda q, *_: (q,) + (0,) * (len(shape) - 1))

    def mine(shape):
        return pl.BlockSpec(shape, lambda q, s, m: (m[0],) + (0,) * (len(shape) - 1))

    def by_slot(shape):
        return pl.BlockSpec(shape, lambda q, s, m: (s[q],) + (0,) * (len(shape) - 1))

    state, tail = (1, 8, 128, 128), (1, 3, 3072)
    ff = w_gate.shape[-1]
    return pl.pallas_call(
        finish_kernel,
        name="finish",
        grid_spec=pltpu.PrefetchScalarGridSpec(
            num_scalar_prefetch=2,
            grid=(4,),
            in_specs=[
                whole((256, 1024)), whole((256, 1024)), whole((1, 1024)), whole((4, 1024, 256)),
                by_step((1, 1024, ff)), by_step((1, 1024, ff)), by_step((1, 1024, ff)),
                by_step(state), by_step(state), by_step(tail),
                mine(state), mine(state), mine(tail),
            ],
            out_specs=[whole((256, 1024)), by_slot(state), by_slot(state), by_slot(tail)],
            scratch_shapes=[
                pltpu.VMEM((256, 1024), jnp.float32),
                pltpu.VMEM((256, 1024), jnp.bfloat16),
                pltpu.VMEM((256, 1024), jnp.float32),
            ],
        ),
        out_shape=[
            jax.ShapeDtypeStruct((256, 1024), jnp.bfloat16),
            jax.ShapeDtypeStruct((4, 8, 128, 128), jnp.float32),
            jax.ShapeDtypeStruct((4, 8, 128, 128), jnp.float32),
            jax.ShapeDtypeStruct((4, 3, 3072), jnp.bfloat16),
        ],
        compiler_params=pltpu.CompilerParams(vmem_limit_bytes=60 << 20),
    )(slots, me, readout, tokens, gain, w_out, w_gate, w_up, w_down, *got, *own)


def shards(
    tokens, lengths, ridge_keys, ridge_values, conv_tail, page_table, w_qkv, conv_weight, w_gates,
    decay_rate, ridge, w_out, attn_gain, ffn_gain, w_gate, w_up, w_down,
):
    requests, length, width = tokens.shape
    flat = tokens.reshape(requests * length, width)
    pieces = jnp.concatenate(
        [w_qkv.reshape(4, 4, 768).swapaxes(0, 1), w_out.reshape(4, 4, 256).swapaxes(0, 1)], axis=2
    )
    pages = jnp.broadcast_to(page_table[None, :], (8, requests))
    pages = jnp.pad(pages, ((0, 0), (0, 128 - requests)))
    *weights, all_pages = gather_all(pieces, pages, w_gate, w_up, w_down.T)
    qa, qb, qc, wo, wg, wu, wd = [w.reshape(4, 1024, w.shape[-1]) for w in weights]
    me = lax.axis_index("mesh").astype(jnp.int32)
    group = all_pages[:, 0, :requests]
    slots = jnp.sum(jnp.where(group // requests == me, group % requests, 0), axis=1)
    readout, *own = mesa(
        lengths, page_table // requests, ridge, flat, w_gates, attn_gain[None, :],
        decay_rate[None, :], conv_weight, conv_tail, ridge_keys, ridge_values, (qa, qb, qc),
    )
    got = handover(*own)
    mixed, keys, values, tails = finish(
        slots, me[None], readout, flat, ffn_gain[None, :], wo, wg, wu, wd, got, own
    )
    return (
        mixed.reshape(tokens.shape), keys, values, tails, readout.reshape(requests, length, -1)
    )


def solution(mesh):
    both = ("req", "mesh")
    in_specs = (
        P(both, None, None), P(both), P(both, None, None, None), P(both, None, None, None),
        P(both, None, None), P(both), P(both, None), P(), P(), P(), P(), P(both, None), P(), P(),
        P("req", "mesh"), P("req", "mesh"), P("mesh", "req"),
    )
    out_specs = (
        P(both, None, None), P(both, None, None, None), P(both, None, None, None),
        P(both, None, None), P(both, None, None),
    )
    return jax.shard_map(shards, mesh=mesh, in_specs=in_specs, out_specs=out_specs, check_vma=False)
```

```python
import functools

import jax
import jax.numpy as jnp
from jax import lax
from jax.experimental import pallas as pl
from jax.experimental.pallas import tpu as pltpu
from jax.sharding import PartitionSpec as P

ITERS = 5
MESH = pl.DeviceIdType.MESH
ANY = pl.BlockSpec(memory_space=pl.ANY)
VMEM = pl.BlockSpec(memory_space=pltpu.VMEM)
NX, NY, NZ, ZH = 4, 4, 8, 4
ALL = None


def place_of():
    req = lax.axis_index("req")
    peer = lax.axis_index("mesh")
    x = req // (NY * ZH)
    y = (req // ZH) % NY
    z = (req % ZH) * 2 + peer // 2
    return x, y, z, peer % 2


def device_of(x, y, z, core):
    return ((x * NY + y) * ZH + z // 2, (z % 2) * 2 + core)


def slab(ref, core, x, y, z, half=None):
    lo, hi = (slice(0, 2), slice(0, ZH)) if z is ALL else (z % 2, z // 2)
    xs = slice(0, NX) if x is ALL else x
    ys = slice(0, NY) if y is ALL else y
    if half is not None:
        if z is ALL:
            lo = slice(half, half + 1)
        else:
            xs = slice(2 * half, 2 * half + 2)
    return ref.at[core, lo, xs, ys, hi]


class Gather:
    def __init__(self, dest, order, sems, base, me):
        self.dest, self.order, self.sems, self.next, self.me = dest, order, sems, base, me
        self.sent = []

    def send(self, where, target):
        x, y, z, core = target
        at = self.next
        self.next += 1
        copy = pltpu.make_async_remote_copy(
            src_ref=where,
            dst_ref=where,
            send_sem=self.sems.at[0, at],
            recv_sem=self.sems.at[1, at],
            device_id=device_of(x, y, z, core),
            device_id_type=MESH,
        )
        copy.start()
        self.sent.append(copy)
        return at

    def arrive(self, where, at):
        pltpu.make_async_remote_copy(
            src_ref=where,
            dst_ref=where,
            send_sem=self.sems.at[0, at],
            recv_sem=self.sems.at[1, at],
            device_id=device_of(*self.me),
            device_id_type=MESH,
        ).wait_recv()

    def moved(self, axis, by):
        place = list(self.me)
        size = (NX, NY, NZ)[axis]
        place[axis] = lax.rem(place[axis] + by + size, size)
        return tuple(place)

    def part(self, axis, by, done, half=None, core=None):
        place = list(self.moved(axis, by))
        for each in done:
            place[each] = ALL
        x, y, z, own = place
        return slab(self.dest, own if core is None else core, x, y, z, half)

    def partner(self):
        x, y, z, core = self.me
        return (x, y, z, 1 - core)

    def stages(self):
        out = []
        first, second, third = self.order
        state = {}

        def direct():
            size = (NX, NY, NZ)[first]
            state["first"] = [
                (by, self.send(self.part(first, 0, ()), self.moved(first, by)))
                for by in range(1, size)
            ]

        def ring(axis, done, last):
            size = (NX, NY, NZ)[axis]
            far = size // 2
            tag = ("ring", axis)

            def cross(by, half):
                if last:
                    at = self.send(self.part(axis, by, done, half), self.partner())
                    state.setdefault("cross", []).append((by, half, at))

            def begin():
                here = self.part(axis, 0, done)
                state[tag] = [
                    (self.send(here, self.moved(axis, 1)), self.send(here, self.moved(axis, -1)))
                ]
                cross(0, None)

            def middle(step):
                right, left = state[tag][-1]
                cut = step == far - 1
                self.arrive(self.part(axis, -step, done), right)
                at_right = self.send(
                    self.part(axis, -step, done, 0 if cut else None), self.moved(axis, 1)
                )
                self.arrive(self.part(axis, step, done), left)
                at_left = self.send(
                    self.part(axis, step, done, 1 if cut else None), self.moved(axis, -1)
                )
                state[tag].append((at_right, at_left))
                cross(-step, None)
                cross(step, None)

            def end():
                right, left = state[tag][-1]
                self.arrive(self.part(axis, far, done, 0), right)
                cross(far, 0)
                self.arrive(self.part(axis, far, done, 1), left)
                cross(far, 1)

            return begin, [functools.partial(middle, s) for s in range(1, far)], end

        b2, m2, e2 = ring(second, (first,), False)
        b3, m3, e3 = ring(third, (first, second), True)

        def after_first():
            for by, at in state["first"]:
                self.arrive(self.part(first, -by, ()), at)
            b2()

        def after_second():
            e2()
            b3()

        def after_cross():
            for by, half, at in state["cross"]:
                self.arrive(
                    self.part(third, by, (first, second), half, core=1 - self.me[3]), at
                )
            for copy in self.sent:
                copy.wait_send()

        out.append(direct)
        out.append(after_first)
        out.extend(m2)
        out.append(after_second)
        out.extend(m3)
        out.append(e3)
        out.append(after_cross)
        return out


COPIES = 26
XYZ, ZYX, ZXY = (0, 1, 2), (2, 1, 0), (2, 0, 1)


def enter(me, group=True):
    barrier = pltpu.get_barrier_semaphore()
    x, y, z, core = me
    others = [(lax.rem(x + by, NX), y, z, core) for by in range(1, NX)]
    others += [(x, lax.rem(y + by, NY), z, core) for by in range(1, NY)]
    others += [(x, y, lax.rem(z + by, NZ), core) for by in range(1, NZ)]
    others += [(x, y, z, 1 - core)]
    if group:
        pair = (z // 2) * 2 + 1 - z % 2
        others += [(x, y, pair, 1 - core)]
    for other in others:
        pl.semaphore_signal(barrier, inc=1, device_id=device_of(*other), device_id_type=MESH)
    pl.semaphore_wait(barrier, len(others))


def run_stages(jobs):
    lists = [job.stages() for job in jobs]
    for step in range(max(len(each) for each in lists)):
        for each in lists:
            if step < len(each):
                each[step]()


def gather_kernel(
    pieces_ref, pages_ref, gate_ref, up_ref, down_ref,
    qa, qb, qc, wo, wg, wu, wd, pages_out,
    landed, rows, stage, sems, group_sems, local_sems,
):
    me = place_of()
    x, y, z, core = me
    req, peer = lax.axis_index("req"), lax.axis_index("mesh")
    enter(me)
    early = []
    for by in range(1, 4):
        other = lax.rem(peer + by, 4)
        for what, (src, dst) in enumerate(
            (
                (pieces_ref.at[other], landed.at[peer]),
                (pages_ref, pages_out.at[peer]),
            )
        ):
            copy = pltpu.make_async_remote_copy(
                src_ref=src,
                dst_ref=dst,
                send_sem=group_sems.at[0, what, by],
                recv_sem=group_sems.at[1, what, by],
                device_id=(req, other),
                device_id_type=MESH,
            )
            copy.start()
            early.append(copy)
    lo, hi = z % 2, z // 2
    own = [
        pltpu.make_async_copy(pages_ref, pages_out.at[peer], local_sems.at[0]),
        pltpu.make_async_copy(gate_ref, wg.at[core, lo, x, y, hi], local_sems.at[1]),
        pltpu.make_async_copy(up_ref, wu.at[core, lo, x, y, hi], local_sems.at[2]),
        pltpu.make_async_copy(down_ref, wd.at[core, lo, x, y, hi], local_sems.at[3]),
        pltpu.make_async_copy(pieces_ref.at[peer], landed.at[peer], local_sems.at[4]),
    ]
    for copy in own:
        copy.start()
    own[4].wait()
    for by in range(1, 4):
        source = lax.rem(peer + 4 - by, 4)
        for what, where in enumerate((landed.at[source], pages_out.at[source])):
            pltpu.make_async_remote_copy(
                src_ref=where,
                dst_ref=where,
                send_sem=group_sems.at[0, what, by],
                recv_sem=group_sems.at[1, what, by],
                device_id=(req, peer),
                device_id_type=MESH,
            ).wait_recv()
    for source in range(4):
        rows[4 * source : 4 * source + 4, :] = landed[source].astype(jnp.float32)
    stage[...] = rows[...].astype(jnp.bfloat16)
    blocks = [
        pltpu.make_async_copy(
            stage.at[:, 256 * n : 256 * n + 256],
            ref.at[core, lo, x, y, hi],
            local_sems.at[5 + n],
        )
        for n, ref in enumerate((qa, qb, qc, wo))
    ]
    for copy in blocks:
        copy.start()
    for copy in blocks:
        copy.wait()
    for copy in own[:4]:
        copy.wait()
    run_stages(
        [
            Gather(ref, order, sems.at[n], 0, me)
            for n, (ref, order) in enumerate(
                (
                    (qa, XYZ), (qb, ZYX), (qc, ZXY), (wg, XYZ), (wu, ZYX), (wd, ZXY), (wo, ZXY),
                )
            )
        ]
    )
    for copy in early:
        copy.wait_send()


def gather_all(pieces, pages, gate, up, down):
    grid = (2, 2, NX, NY, ZH, 16)

    def block(n):
        return jax.ShapeDtypeStruct(grid + (n,), jnp.bfloat16)

    ff = gate.shape[1]
    return pl.pallas_call(
        gather_kernel,
        name="gather_weights",
        out_shape=[block(256)] * 4
        + [block(ff)] * 3
        + [jax.ShapeDtypeStruct((4,) + pages.shape, jnp.int32)],
        in_specs=[VMEM] * 5,
        out_specs=[ANY] * 8,
        scratch_shapes=[
            pltpu.VMEM((4, 4, 1024), jnp.bfloat16),
            pltpu.VMEM((16, 1024), jnp.float32),
            pltpu.VMEM((16, 1024), jnp.bfloat16),
            pltpu.SemaphoreType.DMA((7, 2, COPIES)),
            pltpu.SemaphoreType.DMA((2, 2, 4)),
            pltpu.SemaphoreType.DMA((9,)),
        ],
        compiler_params=pltpu.CompilerParams(collective_id=0, has_side_effects=True),
    )(pieces, pages, gate, up, down)


def split2(value):
    high = value.astype(jnp.bfloat16)
    low = (value - high.astype(jnp.float32)).astype(jnp.bfloat16)
    return jnp.concatenate([high, low], axis=0)


def dot(a, b, contract=((1,), (0,)), precision=None):
    return lax.dot_general(
        a, b, (contract, ((), ())), preferred_element_type=jnp.float32, precision=precision
    )


def dot2(stacked, b, contract=((1,), (0,))):
    both = dot(stacked, b, contract)
    half = both.shape[0] // 2
    return both[:half] + both[half:]


def rms_norm(values, gain):
    return values * lax.rsqrt(jnp.mean(values * values, axis=-1, keepdims=True) + 1e-05) * gain


def statistics_kernel(
    lengths, dest,
    tokens, w_gates, gain, rate, conv_weight, tail, keys0, values0, qa, qb, qc,
    act, sums, rows, send_keys, send_values, send_tail,
    normed, projected, extended,
):
    r = pl.program_id(0)
    high = lax.Precision.HIGHEST

    @pl.when(r == 0)
    def _():
        normed[...] = rms_norm(tokens[...].astype(jnp.float32), gain[...]).astype(jnp.bfloat16)
        for core in range(2):
            for lo in range(2):
                for n, ref in enumerate((qa, qb, qc)):
                    at = (lo * 2 + core) * 768 + n * 256
                    projected[:, at : at + 256] = dot(
                        normed[...], ref[core * 2 + lo]
                    ).astype(jnp.bfloat16)

    length = lengths[r]
    mine = pl.ds(pl.multiple_of(r * 64, 64), 64)
    extended[5:8, :] = tail[0].astype(jnp.float32)
    extended[8:72, :] = projected[mine, :].astype(jnp.float32)
    from_row = 5 + length
    window = extended[pl.ds(pl.multiple_of(from_row // 8 * 8, 8), 16), :]
    send_tail[0] = pltpu.roll(window, (16 - from_row % 8) % 16, 0)[:3].astype(jnp.bfloat16)
    total = conv_weight[0:1, :] * extended[5:69, :]
    for tap in range(1, 4):
        total = total + conv_weight[tap : tap + 1, :] * extended[5 + tap : 69 + tap, :]
    act[...] = total * jax.nn.sigmoid(total)

    logits = dot(normed[mine, :], w_gates[...])
    pick_row = lax.broadcasted_iota(jnp.int32, (16, 8), 0)
    pick_col = lax.broadcasted_iota(jnp.int32, (16, 8), 1)
    in_logit = dot(logits, (pick_row == 2 * pick_col).astype(jnp.float32), precision=high)
    out_logit = dot(logits, (pick_row == 2 * pick_col + 1).astype(jnp.float32), precision=high)
    slot = lax.broadcasted_iota(jnp.int32, (64, 8), 0)
    live = (slot < length).astype(jnp.float32)
    beta = jax.nn.sigmoid(in_logit) * live
    log_decay = -rate[...] * jax.nn.softplus(out_logit) * live
    t_at = lax.broadcasted_iota(jnp.int32, (64, 64), 0)
    s_at = lax.broadcasted_iota(jnp.int32, (64, 64), 1)
    lower = (s_at <= t_at).astype(jnp.float32)
    same = (t_at == s_at).astype(jnp.float32)
    cum = dot(lower, log_decay, precision=high)
    cum_rows = dot(cum, same, ((0,), (0,)), precision=high)
    beta_rows = dot(beta, same, ((0,), (0,)), precision=high)
    sums[...] = cum
    rows[0, 0:8, :] = cum_rows
    rows[0, 8:16, :] = beta_rows

    for h in range(8):
        q_at = slice(h * 128, h * 128 + 128)
        k_at = slice(1024 + h * 128, 1152 + h * 128)
        q, k = act[:, q_at], act[:, k_at]
        v = act[:, 2048 + h * 128 : 2176 + h * 128]
        act[:, q_at] = q * lax.rsqrt(jnp.sum(q * q, axis=-1, keepdims=True) + 1e-06)
        k = k * lax.rsqrt(jnp.sum(k * k, axis=-1, keepdims=True) + 1e-06)
        act[:, k_at] = k
        last = cum[63:64, h : h + 1]
        final = jnp.exp(last)
        tail_row = jnp.exp(last - cum_rows[h : h + 1, :]) * beta_rows[h : h + 1, :]
        k_b = k.astype(jnp.bfloat16)
        send_keys[0, h] = (
            final * keys0[0, h] + dot2(split2(k.T * tail_row), k_b)
        ).astype(jnp.bfloat16)
        send_values[0, h] = (
            final * values0[0, h] + dot2(split2(v.T * tail_row), k_b)
        ).astype(jnp.bfloat16)


HEADS_AT_ONCE = 4


def by_request(shape):
    return pl.BlockSpec(shape, lambda r, *_: (r,) + (0,) * (len(shape) - 1))


def whole(shape):
    return pl.BlockSpec(shape, lambda r, *_: (0,) * len(shape))


STATE = (1, 8, 128, 128)


def statistics(lengths, dest, tokens, w_gates, gain, rate, conv_weight, tail, keys0, values0, qs):
    def by_dest(shape):
        return pl.BlockSpec(shape, lambda r, n, d: (d[r],) + (0,) * (len(shape) - 1))

    return pl.pallas_call(
        statistics_kernel,
        name="statistics",
        grid_spec=pltpu.PrefetchScalarGridSpec(
            num_scalar_prefetch=2,
            grid=(4,),
            in_specs=[
                whole((256, 1024)), whole((1024, 16)), whole((1, 1024)), whole((1, 8)),
                whole((4, 3072)), by_request((1, 3, 3072)), by_request(STATE),
                by_request(STATE), whole((4, 1024, 256)), whole((4, 1024, 256)),
                whole((4, 1024, 256)),
            ],
            out_specs=[
                by_request((64, 3072)), by_request((64, 8)), by_request((1, 16, 64)),
                by_dest(STATE), by_dest(STATE), by_dest((1, 3, 3072)),
            ],
            scratch_shapes=[
                pltpu.VMEM((256, 1024), jnp.bfloat16),
                pltpu.VMEM((256, 3072), jnp.bfloat16),
                pltpu.VMEM((80, 3072), jnp.float32),
            ],
        ),
        out_shape=[
            jax.ShapeDtypeStruct((256, 3072), jnp.float32),
            jax.ShapeDtypeStruct((256, 8), jnp.float32),
            jax.ShapeDtypeStruct((4, 16, 64), jnp.float32),
            jax.ShapeDtypeStruct((4, 8, 128, 128), jnp.bfloat16),
            jax.ShapeDtypeStruct((4, 8, 128, 128), jnp.bfloat16),
            jax.ShapeDtypeStruct((4, 3, 3072), jnp.bfloat16),
        ],
        compiler_params=pltpu.CompilerParams(vmem_limit_bytes=60 << 20),
    )(lengths, dest, tokens, w_gates, gain, rate, conv_weight, tail, keys0, values0, *qs)


def handover_copies(sent, got, sems):
    req, peer = lax.axis_index("req"), lax.axis_index("mesh")
    return [
        pltpu.make_async_remote_copy(
            src_ref=src.at[lax.rem(peer + by, 4)],
            dst_ref=dst.at[peer],
            send_sem=sems.at[0, by, n],
            recv_sem=sems.at[1, by, n],
            device_id=(req, lax.rem(peer + by, 4)),
            device_id_type=MESH,
        )
        for by in range(1, 4)
        for n, (src, dst) in enumerate(zip(sent, got))
    ]


def solve_kernel(
    act, sums, rows, ridge, keys0, values0, keys, values, tails,
    readout, got_keys, got_values, got_tails,
    sems,
):
    r = pl.program_id(0)
    req, peer = lax.axis_index("req"), lax.axis_index("mesh")
    sent, got = (keys, values, tails), (got_keys, got_values, got_tails)

    @pl.when(r == 0)
    def _():
        barrier = pltpu.get_barrier_semaphore()
        for by in range(1, 4):
            pl.semaphore_signal(
                barrier, inc=1, device_id=(req, lax.rem(peer + by, 4)), device_id_type=MESH
            )
        pl.semaphore_wait(barrier, 3)
        for copy in handover_copies(sent, got, sems):
            copy.start()

    t_at = lax.broadcasted_iota(jnp.int32, (64, 64), 0)
    s_at = lax.broadcasted_iota(jnp.int32, (64, 64), 1)
    causal = s_at <= t_at
    cum = sums[...]
    carried_all = jnp.exp(cum)
    for first in range(0, 8, HEADS_AT_ONCE):
        heads = range(first, first + HEADS_AT_ONCE)
        states = []
        for h in heads:
            q = act[:, h * 128 : h * 128 + 128]
            k = act[:, 1024 + h * 128 : 1152 + h * 128]
            v = act[:, 2048 + h * 128 : 2176 + h * 128]
            spread = jnp.exp(jnp.minimum(cum[:, h : h + 1] - rows[0, h : h + 1, :], 0.0))
            weight = jnp.where(causal, spread, 0.0) * rows[0, 8 + h : 9 + h, :]
            k_tb = k.T.astype(jnp.bfloat16)
            states.append(
                dict(
                    x=jnp.zeros_like(q), res=q, p=q, rr=jnp.sum(q * q, axis=-1, keepdims=True),
                    right=jnp.concatenate([keys0[0, h].astype(jnp.bfloat16), k_tb], axis=1),
                    k_b=k.astype(jnp.bfloat16), k_tb=k_tb, v_b=v.astype(jnp.bfloat16),
                    v0=values0[0, h].astype(jnp.bfloat16), weight=weight,
                    carried=carried_all[:, h : h + 1], ridge=ridge[:, h : h + 1],
                )
            )
        for _ in range(ITERS):
            for s in states:
                both = dot2(split2(s["p"]), s["right"])
                s["start"] = s["carried"] * both[:, :128]
                s["scores"] = both[:, 128:] * s["weight"]
            for s in states:
                applied = (
                    s["start"] + dot2(split2(s["scores"]), s["k_b"]) + s["ridge"] * s["p"]
                )
                step = s["rr"] / (jnp.sum(s["p"] * applied, axis=-1, keepdims=True) + 1e-20)
                s["x"] = s["x"] + step * s["p"]
                s["res"] = s["res"] - step * applied
                after = jnp.sum(s["res"] * s["res"], axis=-1, keepdims=True)
                s["p"] = s["res"] + after / (s["rr"] + 1e-20) * s["p"]
                s["rr"] = after
        for h, s in zip(heads, states):
            stacked = split2(s["x"])
            start = s["carried"] * dot2(stacked, s["v0"], ((1,), (1,)))
            scores = dot2(stacked, s["k_tb"]) * s["weight"]
            readout[:, h * 128 : h * 128 + 128] = (
                start + dot2(split2(scores), s["v_b"])
            ).astype(jnp.bfloat16)

    @pl.when(r == 3)
    def _():
        for by in range(1, 4):
            source = lax.rem(peer + 4 - by, 4)
            for n, dst in enumerate(got):
                pltpu.make_async_remote_copy(
                    src_ref=dst.at[source],
                    dst_ref=dst.at[source],
                    send_sem=sems.at[0, by, n],
                    recv_sem=sems.at[1, by, n],
                    device_id=(req, peer),
                    device_id_type=MESH,
                ).wait_recv()
        for copy in handover_copies(sent, got, sems):
            copy.wait_send()


def solve(act, sums, rows, ridge, keys0, values0, own):
    return pl.pallas_call(
        solve_kernel,
        name="solve",
        grid=(4,),
        in_specs=[
            by_request((64, 3072)), by_request((64, 8)), by_request((1, 16, 64)),
            whole((1, 8)), by_request(STATE), by_request(STATE), ANY, ANY, ANY,
        ],
        out_specs=[by_request((64, 1024)), ANY, ANY, ANY],
        out_shape=[jax.ShapeDtypeStruct((256, 1024), jnp.bfloat16)]
        + [jax.ShapeDtypeStruct(a.shape, a.dtype) for a in own],
        scratch_shapes=[pltpu.SemaphoreType.DMA((2, 4, 3))],
        compiler_params=pltpu.CompilerParams(
            collective_id=1, has_side_effects=True, vmem_limit_bytes=60 << 20
        ),
    )(act, sums, rows, ridge, keys0, values0, *own)


def finish_kernel(
    slots, me,
    readout, tokens, gain, w_out, w_gate, w_up, w_down,
    got_keys, got_values, got_tails, own_keys, own_values, own_tails,
    mixed, keys, values, tails,
    after, ffn_in, total,
):
    q = pl.program_id(0)

    @pl.when(q == 0)
    def _():
        for core in range(2):
            for lo in range(2):
                at = (lo * 2 + core) * 256
                after[:, at : at + 256] = (
                    tokens[:, at : at + 256].astype(jnp.float32)
                    + dot(readout[...], w_out[core * 2 + lo])
                ).astype(jnp.bfloat16).astype(jnp.float32)
        ffn_in[...] = rms_norm(after[...], gain[...]).astype(jnp.bfloat16)

    gate = dot(ffn_in[...], w_gate[0])
    hidden = (gate * jax.nn.sigmoid(gate) * dot(ffn_in[...], w_up[0])).astype(jnp.bfloat16)
    part = dot(hidden, w_down[0], ((1,), (1,)))

    @pl.when(q == 0)
    def _():
        total[...] = part

    @pl.when(jnp.logical_and(q > 0, q < 3))
    def _():
        total[...] += part

    @pl.when(q == 3)
    def _():
        mixed[...] = (after[...] + (total[...] + part)).astype(jnp.bfloat16)

    mine = me[0] == q
    keys[...] = jnp.where(mine, own_keys[...], got_keys[...]).astype(jnp.float32)
    values[...] = jnp.where(mine, own_values[...], got_values[...]).astype(jnp.float32)
    tails[...] = jnp.where(mine, own_tails[...], got_tails[...])


def finish(slots, me, readout, tokens, gain, w_out, w_gate, w_up, w_down, got, own):
    def whole(shape):
        return pl.BlockSpec(shape, lambda q, *_: (0,) * len(shape))

    def by_step(shape):
        return pl.BlockSpec(shape, lambda q, *_: (q,) + (0,) * (len(shape) - 1))

    def mine(shape):
        return pl.BlockSpec(shape, lambda q, s, m: (m[0],) + (0,) * (len(shape) - 1))

    def by_slot(shape):
        return pl.BlockSpec(shape, lambda q, s, m: (s[q],) + (0,) * (len(shape) - 1))

    state, tail = (1, 8, 128, 128), (1, 3, 3072)
    ff = w_gate.shape[-1]
    return pl.pallas_call(
        finish_kernel,
        name="finish",
        grid_spec=pltpu.PrefetchScalarGridSpec(
            num_scalar_prefetch=2,
            grid=(4,),
            in_specs=[
                whole((256, 1024)), whole((256, 1024)), whole((1, 1024)), whole((4, 1024, 256)),
                by_step((1, 1024, ff)), by_step((1, 1024, ff)), by_step((1, 1024, ff)),
                by_step(state), by_step(state), by_step(tail),
                mine(state), mine(state), mine(tail),
            ],
            out_specs=[whole((256, 1024)), by_slot(state), by_slot(state), by_slot(tail)],
            scratch_shapes=[
                pltpu.VMEM((256, 1024), jnp.float32),
                pltpu.VMEM((256, 1024), jnp.bfloat16),
                pltpu.VMEM((256, 1024), jnp.float32),
            ],
        ),
        out_shape=[
            jax.ShapeDtypeStruct((256, 1024), jnp.bfloat16),
            jax.ShapeDtypeStruct((4, 8, 128, 128), jnp.float32),
            jax.ShapeDtypeStruct((4, 8, 128, 128), jnp.float32),
            jax.ShapeDtypeStruct((4, 3, 3072), jnp.bfloat16),
        ],
        compiler_params=pltpu.CompilerParams(vmem_limit_bytes=60 << 20),
    )(slots, me, readout, tokens, gain, w_out, w_gate, w_up, w_down, *got, *own)


def shards(
    tokens, lengths, ridge_keys, ridge_values, conv_tail, page_table, w_qkv, conv_weight, w_gates,
    decay_rate, ridge, w_out, attn_gain, ffn_gain, w_gate, w_up, w_down,
):
    requests, length, width = tokens.shape
    flat = tokens.reshape(requests * length, width)
    pieces = jnp.concatenate(
        [w_qkv.reshape(4, 4, 768).swapaxes(0, 1), w_out.reshape(4, 4, 256).swapaxes(0, 1)], axis=2
    )
    pages = jnp.broadcast_to(page_table[None, :], (8, requests))
    pages = jnp.pad(pages, ((0, 0), (0, 128 - requests)))
    *weights, all_pages = gather_all(pieces, pages, w_gate, w_up, w_down.T)
    qa, qb, qc, wo, wg, wu, wd = [w.reshape(4, 1024, w.shape[-1]) for w in weights]
    me = lax.axis_index("mesh").astype(jnp.int32)
    group = all_pages[:, 0, :requests]
    slots = jnp.sum(jnp.where(group // requests == me, group % requests, 0), axis=1)
    act, sums, rows, *own = statistics(
        lengths, page_table // requests, flat, w_gates, attn_gain[None, :], decay_rate[None, :],
        conv_weight, conv_tail, ridge_keys, ridge_values, (qa, qb, qc),
    )
    readout, *got = solve(act, sums, rows, ridge[None, :], ridge_keys, ridge_values, own)
    mixed, keys, values, tails = finish(
        slots, me[None], readout, flat, ffn_gain[None, :], wo, wg, wu, wd, got, own
    )
    return (
        mixed.reshape(tokens.shape), keys, values, tails, readout.reshape(requests, length, -1)
    )


def solution(mesh):
    both = ("req", "mesh")
    in_specs = (
        P(both, None, None), P(both), P(both, None, None, None), P(both, None, None, None),
        P(both, None, None), P(both), P(both, None), P(), P(), P(), P(), P(both, None), P(), P(),
        P("req", "mesh"), P("req", "mesh"), P("mesh", "req"),
    )
    out_specs = (
        P(both, None, None), P(both, None, None, None), P(both, None, None, None),
        P(both, None, None), P(both, None, None),
    )
    return jax.shard_map(shards, mesh=mesh, in_specs=in_specs, out_specs=out_specs, check_vma=False)
```
